512 devices in a mesh: depth: 32 (over x, y), rows: 16 (over z, core).
Axes of the slice: x: 4, y: 8, z: 8, core: 2. Of those that a mesh axis runs over, the one named last changes fastest.
Arguments:
- ref_feat: bfloat16 [2, 32, 5120], P(None, 'rows'), may hold values from -6 to 6
- src_feat: bfloat16 [2, 4, 32, 5120], P(None, None, 'rows'), may hold values from -6 to 6
- block_index: int32 [2, 4, 192, 16], P(None, None, 'depth', 'rows'), may hold values from 0 to 14, as said below
- blend: bfloat16 [2, 4, 192, 32, 160], P(None, None, 'depth', 'rows'), may hold values from 0 to 1
- conv_first: bfloat16 [3, 3, 3, 32, 40], replicated, may hold values from -0.1875 to 0.1875
- bias_first: float32 [32], replicated, may hold values from -3 to 3
- conv_second: bfloat16 [3, 3, 3, 32, 32], replicated, may hold values from -0.21875 to 0.21875
- bias_second: float32 [32], replicated, may hold values from -3 to 3
Outputs:
- regularized: bfloat16 [2, 192, 32, 5120], P(None, 'depth', 'rows')
The draws below stay inside these ranges and needn't reach their ends.
Inputs may be any that keep to these rules, and one draw needn't show every extreme that they name: block_index[b, v, d, q] is q - 1 or q, held within 0 to 14, so rows of block q blend source row blocks block_index and block_index + 1.
All inputs are finite; a program needn't handle non-finite values.
Results may differ from the reference program's by a relative error of at most 0.0046.
Values may be sent and summed in bfloat16 or wider, within the bound.
No kernel may reach another device: no remote copies, remote signals or barrier semaphores. Data moves between devices by JAX's collectives and lax.ppermute only.
A program may use at most 64 MiB of HBM per device.

```python
import jax
import jax.numpy as jnp
from jax import lax

FEAT = 32
GROUPS = 8
REG = 32
SRC = 4
WIDTH = 160
ROWS_DEV = 2
BATCH = 2
D = 192
H = 32
NB = 16


def draw_block_index(key, part):
    offset = jax.random.randint(key, (BATCH, SRC, D, NB), -1, 1, dtype=jnp.int32)
    blocks = jnp.arange(NB, dtype=jnp.int32)
    return jnp.clip(blocks + offset, 0, NB - 2).astype(jnp.int32)


def steps_of(key, extent, cuts, least, top_value):
    loudness = 1.0
    for dim, blocks in cuts:
        heights = jax.random.uniform(jax.random.fold_in(jax.random.fold_in(key, 6), dim), (blocks,), jnp.float32, least / len(cuts), top_value / len(cuts))
        loudness = loudness * jnp.repeat(jnp.exp(heights), extent[dim] // blocks).reshape((-1,) + (1,) * (len(extent) - 1 - dim))
    return loudness


def bell_draw(own_key, shape, deviation, bound, shards=(), held_as=jnp.bfloat16):
    drawn = deviation * jax.random.normal(own_key, shape, jnp.float32)
    if shards:
        drawn = drawn * steps_of(own_key, shape, shards, -0.22, 0.18)
    return jnp.clip(drawn, -bound, bound).astype(held_as)


def setup_inputs(seed: int = 0) -> dict:
    splits = jax.random.split(jax.random.key(seed), 9)
    return {
        "ref_feat": bell_draw(splits[0], (BATCH, H, FEAT * WIDTH), 1.0, 6.0, ((1, 16),)),
        "src_feat": bell_draw(splits[1], (BATCH, SRC, H, FEAT * WIDTH), 1.0, 6.0, ((2, 16),)),
        "block_index": draw_block_index(jax.random.fold_in(splits[8], 71), 0),
        "blend": jnp.clip(1.0 * jax.random.uniform(splits[3], (BATCH, SRC, D, H, WIDTH), jnp.float32) ** steps_of(splits[3], (BATCH, SRC, D, H, WIDTH), ((2, 32), (3, 16)), -0.2, 0.2), 0.0, 1.0).astype(jnp.bfloat16),
        "conv_first": bell_draw(splits[4], (3, 3, 3, REG, GROUPS + FEAT), (27 * (GROUPS + FEAT)) ** -0.5, 0.1875),
        "bias_first": bell_draw(splits[5], (REG,), 0.5, 3.0, (), jnp.float32),
        "conv_second": bell_draw(splits[6], (3, 3, 3, REG, REG), (27 * REG) ** -0.5, 0.21875),
        "bias_second": bell_draw(splits[7], (REG,), 0.5, 3.0, (), jnp.float32),
    }


def cost_plane(ref_rows, top_rows, bottom_rows, weight, feat_count, columns, groups):
    scenes = top_rows.shape[0]
    source_views = top_rows.shape[1]
    row_count = top_rows.shape[2]
    reference_cube = ref_rows.astype(jnp.float32).reshape(scenes, 1, row_count, feat_count, columns)
    blend_weight = weight.astype(jnp.float32)[:, :, :, None, :]
    upper_part = top_rows.astype(jnp.float32).reshape(scenes, source_views, row_count, feat_count, columns)
    lower_part = bottom_rows.astype(jnp.float32).reshape(scenes, source_views, row_count, feat_count, columns)
    warped = blend_weight * upper_part + (1.0 - blend_weight) * lower_part
    average = (reference_cube[:, 0] + jnp.sum(warped, axis=1)) / (source_views + 1.0)
    spread = ((reference_cube[:, 0] - average) ** 2 + jnp.sum((warped - average[:, None]) ** 2, axis=1)) / (source_views + 1.0)
    per_group = feat_count // groups
    products = (reference_cube * warped).reshape(scenes, source_views, row_count, groups, per_group, columns)
    correlation = jnp.sum(products, axis=(1, 4)) / (source_views * per_group * 1.0)
    stacked = jnp.concatenate([correlation, spread], axis=2).astype(jnp.bfloat16)
    return stacked.reshape(scenes, row_count, (groups + feat_count) * columns)


def layer(volume, kernel, shift_bias, rectify):
    scenes = volume.shape[0]
    channels = kernel.shape[4]
    outputs = kernel.shape[3]
    shaped = volume.reshape(scenes, D, H, channels, WIDTH)
    padded = jnp.pad(shaped, ((0, 0), (1, 1), (1, 1), (0, 0), (1, 1)))
    kernel_wide = kernel.astype(jnp.float32)

    def one_plane(plane):
        block = lax.dynamic_slice_in_dim(padded, plane, 3, 1).astype(jnp.float32)
        summed = jnp.zeros((scenes, H, outputs, WIDTH), jnp.float32)
        for tap_depth in range(3):
            for tap_row in range(3):
                for tap_col in range(3):
                    piece = block[:, tap_depth, tap_row:tap_row + H, :, tap_col:tap_col + WIDTH]
                    summed = summed + jnp.einsum("brcw,oc->brow", piece, kernel_wide[tap_depth, tap_row, tap_col], precision=lax.Precision.HIGHEST)
        result = summed + shift_bias.astype(jnp.float32)[None, None, :, None]
        if rectify:
            result = jnp.maximum(result, 0.0)
        return result.astype(jnp.bfloat16).reshape(scenes, H, outputs * WIDTH)

    planes_out = lax.map(one_plane, jnp.arange(D, dtype=jnp.int32))
    return jnp.moveaxis(planes_out, 0, 1)


def reference(ref_feat, src_feat, block_index, blend, conv_first, bias_first, conv_second, bias_second):
    row_block = jnp.arange(H, dtype=jnp.int32) // ROWS_DEV
    within = jnp.arange(H, dtype=jnp.int32) % ROWS_DEV

    def plane_cost(plane):
        chosen = lax.dynamic_index_in_dim(block_index, plane, 2, keepdims=False)[:, :, row_block]
        top_index = (chosen * ROWS_DEV + within).astype(jnp.int32)[..., None]
        bottom_index = (top_index + ROWS_DEV).astype(jnp.int32)
        top_rows = jnp.take_along_axis(src_feat, top_index, axis=2)
        bottom_rows = jnp.take_along_axis(src_feat, bottom_index, axis=2)
        weight = lax.dynamic_index_in_dim(blend, plane, 2, keepdims=False)
        return cost_plane(ref_feat, top_rows, bottom_rows, weight, FEAT, WIDTH, GROUPS)

    cost_planes = lax.map(plane_cost, jnp.arange(D, dtype=jnp.int32))
    volume = jnp.moveaxis(cost_planes, 0, 1)
    hidden = layer(volume, conv_first, bias_first, True)
    return layer(hidden, conv_second, bias_second, False)
```

```python
import functools

import jax
import jax.numpy as jnp
from jax import lax
from jax.experimental import pallas as pl
from jax.experimental.pallas import tpu as pltpu
from jax.sharding import PartitionSpec as P

F32 = jnp.float32
BF16 = jnp.bfloat16


def pack_features(rows, groups, per_group, columns):
    b, v, m, _ = rows.shape
    x = rows.reshape(b, v, m, groups, per_group, columns)
    return x.transpose(1, 4, 3, 0, 2, 5).reshape(v * per_group * groups, b * m * columns)


def pack_blend(weight):
    b, v, p, m, w = weight.shape
    return weight.transpose(2, 1, 0, 3, 4).reshape(p * v, b * m * w)


def compute_kernel(
    own_ref, halo_ref, w1_ref, w2_ref, b1_ref, b2_ref, out_ref,
    src_ref, rf_ref, tm_ref, tp_ref, e0_ref, dm_ref, dp_ref, vf_ref, v_ref, h_ref,
    *, planes, columns, depth_count, row_count,
):
    q = lax.axis_index("rows")
    core = q % 2
    depth = lax.axis_index("depth")
    lanes = 4 * columns
    views = 4
    first = depth == 0
    last = depth == depth_count - 1

    lane = lax.broadcasted_iota(jnp.int32, (1, lanes), 1)
    col = lane % columns
    row_bit = (lane // columns) % 2

    for i in range(2):
        src_ref[i] = halo_ref[0, 128 * i : 128 * i + 128, :]
        src_ref[2 + i] = own_ref[i, 0:128, :]
        src_ref[4 + i] = halo_ref[1, 128 * i : 128 * i + 128, :]
    half = lax.broadcasted_iota(jnp.int32, (8, 128), 1) < 64

    def put_weights(r, row, w, o):
        turned = pltpu.roll(o, 64, 1)
        b0 = jnp.where(half, o, turned)
        b1 = jnp.where(half, turned, o)
        below = jnp.concatenate([b0, b0, o, b1, b1], axis=1) < -0.5
        tm_ref[r, row : row + 8, :] = jnp.where(below, w, 0.0)
        tp_ref[r, row : row + 8, :] = jnp.where(below, 0.0, 1.0 - w)

    for r in range(4):
        if r == 0:
            rest = halo_ref[0, 256:320, :]
        elif r == 3:
            rest = halo_ref[1, 256:320, :]
        else:
            rest = own_ref[r - 1, 128:192, :]
        rest = rest.astype(F32)
        rf_ref[r] = rest[0:32]
        for i in range(planes * views // 8):
            put_weights(r, 8 + 8 * i, rest[32 + 8 * i : 40 + 8 * i], rest[56:64, 128 * i : 128 * i + 128])
        low_row = (352, 320, 336, 368)[r]
        high_row = (368, 320, 336, 352)[r]
        low = halo_ref[0, low_row : low_row + 16, :].astype(F32)
        high = halo_ref[1, high_row : high_row + 16, :].astype(F32)
        put_weights(r, 0, low[0:8], low[8:16, 0:128])
        put_weights(r, 8 + planes * views, high[0:8], high[8:16, 0:128])

    for k in range(3):
        base = rf_ref[core + k]
        for v in range(views):
            rows = slice(32 * v, 32 * v + 32)
            middle = src_ref[core + k + 1, rows, :].astype(F32)
            e0_ref[k, v] = middle - base
            dm_ref[k, v] = src_ref[core + k, rows, :].astype(F32) - middle
            dp_ref[k, v] = src_ref[core + k + 2, rows, :].astype(F32) - middle

    def volume_plane(pair, carry):
        outside = ((pair == 0) & first) | ((pair == planes // 2 + 1) & last)
        row = pl.multiple_of(pair * 8, 8)
        for k in range(3):
            missing = outside | ((k == 0) & (q == 0)) | ((k == 2) & (q == row_count - 1))
            keep = jnp.where(missing, 0.0, 1.0).astype(F32)
            for i in range(lanes // 128):
                cols = slice(128 * i, 128 * i + 128)
                tm = tm_ref[core + k, pl.ds(row, 8), cols]
                tp = tp_ref[core + k, pl.ds(row, 8), cols]
                base = rf_ref[core + k, :, cols]
                for t in range(2):
                    total = jnp.zeros((32, 128), F32)
                    squares = jnp.zeros((32, 128), F32)
                    for v in range(views):
                        n = views * t + v
                        e = e0_ref[k, v, :, cols] + tm[n : n + 1] * dm_ref[k, v, :, cols]
                        e = e + tp[n : n + 1] * dp_ref[k, v, :, cols]
                        total = total + e
                        squares = squares + e * e
                    spread = squares * (0.2 * keep) - total * total * (0.04 * keep)
                    product = base * (total + 4.0 * base)
                    corr = (product[0:8] + product[8:16] + product[16:24] + product[24:32]) * keep
                    vf_ref[t, k, 0:32, cols] = spread
                    vf_ref[t, k, 32:40, cols] = corr
        for t in range(2):
            p = 2 * pair + t
            for k in range(3):
                v_ref[p, 96 * k : 96 * k + 48, :] = vf_ref[t, k].astype(BF16)
            for k in range(2):
                mixed = jnp.where(
                    row_bit == 0,
                    pltpu.roll(vf_ref[t, k], lanes - columns, 1),
                    pltpu.roll(vf_ref[t, k + 1], columns, 1),
                )
                v_ref[p, 96 * k + 48 : 96 * k + 96, :] = mixed.astype(BF16)
        return carry

    vf_ref[:, :, 40:48, :] = jnp.zeros((2, 3, 8, lanes), F32)
    lax.fori_loop(0, planes // 2 + 2, volume_plane, 0)

    def shifted_sum(parts, width):
        column = jnp.concatenate([col] * (width // lanes), axis=1)
        left = jnp.where(column == 0, 0.0, pltpu.roll(parts[0:32], 1, 1))
        right = jnp.where(column == columns - 1, 0.0, pltpu.roll(parts[64:96], width - 1, 1))
        return parts[32:64] + left + right

    lost = jnp.concatenate(
        [
            jnp.where((row_bit == 0) & (q == 0), 0.0, 1.0),
            jnp.where((row_bit == 1) & (q == row_count - 1), 0.0, 1.0),
        ],
        axis=1,
    )

    def hidden_plane(p, carry):
        upper = jnp.concatenate([v_ref[p + a, 0:144, :] for a in range(3)], axis=0)
        lower = jnp.concatenate([v_ref[p + a, 96:240, :] for a in range(3)], axis=0)
        taps = jnp.concatenate([upper, lower], axis=1)
        parts = jnp.dot(w1_ref[...], taps, preferred_element_type=F32)
        missing = ((p == 0) & first) | ((p == planes + 1) & last)
        keep = lost * jnp.where(missing, 0.0, 1.0).astype(F32)
        hidden = jnp.maximum(shifted_sum(parts, 2 * lanes) + b1_ref[...], 0.0) * keep
        above = hidden[:, :lanes]
        below = hidden[:, lanes:]
        h_ref[p, 0:32, :] = above.astype(BF16)
        h_ref[p, 64:96, :] = below.astype(BF16)
        mixed = jnp.where(row_bit == 0, pltpu.roll(above, lanes - columns, 1), pltpu.roll(below, columns, 1))
        h_ref[p, 32:64, :] = mixed.astype(BF16)
        return carry

    lax.fori_loop(0, planes + 2, hidden_plane, 0)

    def out_plane(p, carry):
        taps = jnp.concatenate([h_ref[p + a] for a in range(3)], axis=0)
        parts = jnp.dot(w2_ref[...], taps, preferred_element_type=F32)
        out_ref[p] = (shifted_sum(parts, lanes) + b2_ref[...]).astype(BF16)
        return carry

    lax.fori_loop(0, planes, out_plane, 0)


def body(ref_feat, src_feat, block_index, blend, conv_first, bias_first, conv_second, bias_second):
    b, v, m, packed = src_feat.shape
    planes, columns = blend.shape[2], blend.shape[4]
    channels = conv_first.shape[4]
    outputs = conv_first.shape[3]
    feat = packed // columns
    groups = channels - feat
    per_group = feat // groups
    depth_count = lax.axis_size("depth")
    row_count = lax.axis_size("rows")
    lanes = b * m * columns
    core = lax.axis_index("rows") % 2

    offset = (block_index[:, :, :, 0] - lax.axis_index("rows")).astype(BF16)
    offset = offset.transpose(2, 1, 0).reshape(planes * v // 8, 8, b, 1)
    offset = jnp.broadcast_to(offset, (planes * v // 8, 8, b, 64)).transpose(1, 0, 2, 3).reshape(8, -1)
    offset = jnp.pad(offset, ((0, 0), (0, lanes - offset.shape[1])))
    own = jnp.concatenate(
        [
            pack_features(src_feat, groups, per_group, columns),
            pack_features(ref_feat[:, None], groups, per_group, columns),
            pack_blend(blend),
            offset,
        ],
        axis=0,
    )
    pairs = [[2 * i, 2 * i + 1] for i in range(row_count // 2)]
    gathered = lax.all_gather(own, "rows", axis_index_groups=pairs)

    def send(x, step_depth, step_chip):
        routes = []
        for d in range(depth_count):
            for r in range(row_count):
                sign = 1 if r % 2 == 0 else -1
                to_d, to_r = d + sign * step_depth, r + 2 * sign * step_chip
                if 0 <= to_d < depth_count and 0 <= to_r < row_count:
                    routes.append((d * row_count + r, to_d * row_count + to_r))
        return lax.ppermute(x, ("depth", "rows"), routes)

    edge_offset = jnp.where(core == 0, gathered[:, 184:192, 256:384], gathered[:, 184:192, 0:128])
    edge_blend = jnp.where(core == 0, gathered[:, 176:184], gathered[:, 160:168])
    edge = jnp.concatenate([edge_blend, jnp.pad(edge_offset, ((0, 0), (0, 0), (0, lanes - 128)))], axis=1)
    from_chip = send(gathered, 0, 1)
    from_depth = send(edge, 1, 0)
    from_same = send(edge, 1, 1)
    from_cross = send(edge, 1, -1)
    halo = jnp.concatenate(
        [
            from_chip[0, 0:128],
            from_chip[1, 0:128],
            lax.dynamic_index_in_dim(from_chip, 1 - core, 0, keepdims=False)[128:192],
            from_depth[0],
            from_depth[1],
            lax.dynamic_index_in_dim(from_same, 1 - core, 0, keepdims=False),
            lax.dynamic_index_in_dim(from_cross, core, 0, keepdims=False),
        ],
        axis=0,
    )
    halos = lax.all_gather(halo, "rows", axis_index_groups=pairs)

    corr = conv_first[..., :groups] * jnp.asarray(0.0625, BF16)
    spread = conv_first[..., groups:].reshape(3, 3, 3, outputs, groups, per_group)
    spread = spread.swapaxes(4, 5).reshape(3, 3, 3, outputs, feat)
    padded = jnp.concatenate([spread, corr, jnp.zeros_like(corr)], axis=-1)
    w1 = padded.transpose(2, 3, 0, 1, 4).reshape(3 * outputs, -1)
    w2 = conv_second.transpose(2, 3, 0, 1, 4).reshape(3 * outputs, -1)

    kernel = functools.partial(
        compute_kernel, planes=planes, columns=columns, depth_count=depth_count, row_count=row_count
    )
    out = pl.pallas_call(
        kernel,
        out_shape=jax.ShapeDtypeStruct((planes, outputs, lanes), BF16),
        in_specs=[pl.BlockSpec(memory_space=pltpu.VMEM)] * 6,
        out_specs=pl.BlockSpec(memory_space=pltpu.VMEM),
        scratch_shapes=[
            pltpu.VMEM((6, 128, lanes), BF16),
            pltpu.VMEM((4, 32, lanes), F32),
            pltpu.VMEM((4, (planes + 4) * v, lanes), F32),
            pltpu.VMEM((4, (planes + 4) * v, lanes), F32),
            pltpu.VMEM((3, v, 32, lanes), F32),
            pltpu.VMEM((3, v, 32, lanes), F32),
            pltpu.VMEM((3, v, 32, lanes), F32),
            pltpu.VMEM((2, 3, 48, lanes), F32),
            pltpu.VMEM((planes + 4, 240, lanes), BF16),
            pltpu.VMEM((planes + 2, 96, lanes), BF16),
        ],
        compiler_params=pltpu.CompilerParams(vmem_limit_bytes=48 * 1024 * 1024),
        name="volume_and_convolutions",
    )(gathered, halos, w1, w2, bias_first[:, None], bias_second[:, None])
    out = out.reshape(planes, outputs, b, m, columns).transpose(2, 0, 3, 1, 4)
    return out.reshape(b, planes, m, outputs * columns)


def solution(mesh):
    in_specs = (
        P(None, "rows", None),
        P(None, None, "rows", None),
        P(None, None, "depth", "rows"),
        P(None, None, "depth", "rows", None),
        P(),
        P(),
        P(),
        P(),
    )
    out_specs = P(None, "depth", "rows", None)
    return jax.shard_map(body, mesh=mesh, in_specs=in_specs, out_specs=out_specs, check_vma=False)
```

```python
import functools

import jax
import jax.numpy as jnp
from jax import lax
from jax.experimental import pallas as pl
from jax.experimental.pallas import tpu as pltpu
from jax.sharding import PartitionSpec as P

F32 = jnp.float32
BF16 = jnp.bfloat16


def pack_features(rows, groups, per_group, columns):
    b, v, m, _ = rows.shape
    x = rows.reshape(b, v, m, groups, per_group, columns)
    return x.transpose(1, 4, 3, 0, 2, 5).reshape(v * per_group * groups, b * m * columns)


def pack_blend(weight):
    b, v, p, m, w = weight.shape
    return weight.transpose(2, 1, 0, 3, 4).reshape(p * v, b * m * w)


def compute_kernel(
    own_ref, far_ref, near_ref, w1_ref, w2_ref, b1_ref, b2_ref, out_ref,
    src_ref, rf_ref, tm_ref, tp_ref, e0_ref, dm_ref, dp_ref, vf_ref, v_ref, h_ref,
    *, planes, columns, depth_count, row_count,
):
    q = lax.axis_index("rows")
    core = q % 2
    depth = lax.axis_index("depth")
    lanes = 4 * columns
    views = 4
    first = depth == 0
    last = depth == depth_count - 1

    lane = lax.broadcasted_iota(jnp.int32, (1, lanes), 1)
    col = lane % columns
    row_bit = (lane // columns) % 2

    src_ref[0] = far_ref[0:128]
    src_ref[1] = near_ref[0]
    src_ref[2] = own_ref[0, 0:128]
    src_ref[3] = own_ref[1, 0:128]
    src_ref[4] = near_ref[1]
    src_ref[5] = far_ref[128:256]
    half = lax.broadcasted_iota(jnp.int32, (8, 128), 1) < 64
    for r in range(4):
        rest = far_ref[256:336] if r in (0, 3) else own_ref[r - 1, 128:208]
        rest = rest.astype(F32)
        rf_ref[r] = rest[0:32]
        for i in range((planes + 4) * views // 8):
            w = rest[32 + 8 * i : 40 + 8 * i]
            o = rest[72:80, 128 * i : 128 * i + 128]
            turned = pltpu.roll(o, 64, 1)
            b0 = jnp.where(half, o, turned)
            b1 = jnp.where(half, turned, o)
            below = jnp.concatenate([b0, b0, o, b1, b1], axis=1) < -0.5
            tm_ref[r, 8 * i : 8 * i + 8, :] = jnp.where(below, w, 0.0)
            tp_ref[r, 8 * i : 8 * i + 8, :] = jnp.where(below, 0.0, 1.0 - w)

    for k in range(3):
        base = rf_ref[core + k]
        for v in range(views):
            rows = slice(32 * v, 32 * v + 32)
            middle = src_ref[core + k + 1, rows, :].astype(F32)
            e0_ref[k, v] = middle - base
            dm_ref[k, v] = src_ref[core + k, rows, :].astype(F32) - middle
            dp_ref[k, v] = src_ref[core + k + 2, rows, :].astype(F32) - middle

    def volume_plane(pair, carry):
        outside = ((pair == 0) & first) | ((pair == planes // 2 + 1) & last)
        row = pl.multiple_of(pair * 8, 8)
        for k in range(3):
            missing = outside | ((k == 0) & (q == 0)) | ((k == 2) & (q == row_count - 1))
            keep = jnp.where(missing, 0.0, 1.0).astype(F32)
            for i in range(lanes // 128):
                cols = slice(128 * i, 128 * i + 128)
                tm = tm_ref[core + k, pl.ds(row, 8), cols]
                tp = tp_ref[core + k, pl.ds(row, 8), cols]
                base = rf_ref[core + k, :, cols]
                for t in range(2):
                    total = jnp.zeros((32, 128), F32)
                    squares = jnp.zeros((32, 128), F32)
                    for v in range(views):
                        n = views * t + v
                        e = e0_ref[k, v, :, cols] + tm[n : n + 1] * dm_ref[k, v, :, cols]
                        e = e + tp[n : n + 1] * dp_ref[k, v, :, cols]
                        total = total + e
                        squares = squares + e * e
                    spread = squares * (0.2 * keep) - total * total * (0.04 * keep)
                    product = base * (total + 4.0 * base)
                    corr = (product[0:8] + product[8:16] + product[16:24] + product[24:32]) * keep
                    vf_ref[t, k, 0:32, cols] = spread
                    vf_ref[t, k, 32:40, cols] = corr
        for t in range(2):
            p = 2 * pair + t
            for k in range(3):
                v_ref[p, 96 * k : 96 * k + 48, :] = vf_ref[t, k].astype(BF16)
            for k in range(2):
                mixed = jnp.where(
                    row_bit == 0,
                    pltpu.roll(vf_ref[t, k], lanes - columns, 1),
                    pltpu.roll(vf_ref[t, k + 1], columns, 1),
                )
                v_ref[p, 96 * k + 48 : 96 * k + 96, :] = mixed.astype(BF16)
        return carry

    vf_ref[:, :, 40:48, :] = jnp.zeros((2, 3, 8, lanes), F32)
    lax.fori_loop(0, planes // 2 + 2, volume_plane, 0)

    def shifted_sum(parts, width):
        column = jnp.concatenate([col] * (width // lanes), axis=1)
        left = jnp.where(column == 0, 0.0, pltpu.roll(parts[0:32], 1, 1))
        right = jnp.where(column == columns - 1, 0.0, pltpu.roll(parts[64:96], width - 1, 1))
        return parts[32:64] + left + right

    lost = jnp.concatenate(
        [
            jnp.where((row_bit == 0) & (q == 0), 0.0, 1.0),
            jnp.where((row_bit == 1) & (q == row_count - 1), 0.0, 1.0),
        ],
        axis=1,
    )

    def hidden_plane(p, carry):
        upper = jnp.concatenate([v_ref[p + a, 0:144, :] for a in range(3)], axis=0)
        lower = jnp.concatenate([v_ref[p + a, 96:240, :] for a in range(3)], axis=0)
        taps = jnp.concatenate([upper, lower], axis=1)
        parts = jnp.dot(w1_ref[...], taps, preferred_element_type=F32)
        missing = ((p == 0) & first) | ((p == planes + 1) & last)
        keep = lost * jnp.where(missing, 0.0, 1.0).astype(F32)
        hidden = jnp.maximum(shifted_sum(parts, 2 * lanes) + b1_ref[...], 0.0) * keep
        above = hidden[:, :lanes]
        below = hidden[:, lanes:]
        h_ref[p, 0:32, :] = above.astype(BF16)
        h_ref[p, 64:96, :] = below.astype(BF16)
        mixed = jnp.where(row_bit == 0, pltpu.roll(above, lanes - columns, 1), pltpu.roll(below, columns, 1))
        h_ref[p, 32:64, :] = mixed.astype(BF16)
        return carry

    lax.fori_loop(0, planes + 2, hidden_plane, 0)

    def out_plane(p, carry):
        taps = jnp.concatenate([h_ref[p + a] for a in range(3)], axis=0)
        parts = jnp.dot(w2_ref[...], taps, preferred_element_type=F32)
        out_ref[p] = (shifted_sum(parts, lanes) + b2_ref[...]).astype(BF16)
        return carry

    lax.fori_loop(0, planes, out_plane, 0)


def body(ref_feat, src_feat, block_index, blend, conv_first, bias_first, conv_second, bias_second):
    b, v, m, packed = src_feat.shape
    planes, columns = blend.shape[2], blend.shape[4]
    channels = conv_first.shape[4]
    outputs = conv_first.shape[3]
    feat = packed // columns
    groups = channels - feat
    per_group = feat // groups
    depth_count = lax.axis_size("depth")
    row_count = lax.axis_size("rows")
    lanes = b * m * columns
    core = lax.axis_index("rows") % 2

    def send(x, step_depth, step_chip, sign_of_core):
        routes = []
        for d in range(depth_count):
            for r in range(row_count):
                sign = sign_of_core[r % 2]
                to_d, to_r = d + sign * step_depth, r + 2 * sign * step_chip
                if 0 <= to_d < depth_count and 0 <= to_r < row_count:
                    routes.append((d * row_count + r, to_d * row_count + to_r))
        return lax.ppermute(x, ("depth", "rows"), routes)

    rows = planes * v
    offset = (block_index[:, :, :, 0] - lax.axis_index("rows")).astype(BF16)
    offset = offset.transpose(2, 1, 0).reshape(rows // 8, 8, b, 1)
    offset = jnp.broadcast_to(offset, (rows // 8, 8, b, 64)).transpose(1, 0, 2, 3).reshape(8, -1)
    weight = pack_blend(blend)

    def edge(i):
        return jnp.concatenate(
            [weight[8 * i : 8 * i + 8], jnp.pad(offset[:, 128 * i : 128 * i + 128], ((0, 0), (0, lanes - 128)))], axis=0
        )

    low = send(edge(rows // 8 - 1), 1, 0, (1, 1))
    high = send(edge(0), 1, 0, (-1, -1))
    own = jnp.concatenate(
        [
            pack_features(src_feat, groups, per_group, columns),
            pack_features(ref_feat[:, None], groups, per_group, columns),
            low[0:8],
            weight,
            high[0:8],
            jnp.concatenate([low[8:16, 0:128], offset, high[8:16, 0:128]], axis=1),
        ],
        axis=0,
    )
    pairs = [[2 * i, 2 * i + 1] for i in range(row_count // 2)]
    gathered = lax.all_gather(own, "rows", axis_index_groups=pairs)
    rest = lax.dynamic_index_in_dim(gathered, 1 - core, 0, keepdims=False)[128:208]
    far = send(jnp.concatenate([gathered[0, 0:128], gathered[1, 0:128], rest], axis=0), 0, 1, (1, -1))
    near = lax.dynamic_slice_in_dim(far, 128 * (1 - core), 128, 0)
    near = lax.all_gather(near, "rows", axis_index_groups=pairs)

    corr = conv_first[..., :groups] * jnp.asarray(0.0625, BF16)
    spread = conv_first[..., groups:].reshape(3, 3, 3, outputs, groups, per_group)
    spread = spread.swapaxes(4, 5).reshape(3, 3, 3, outputs, feat)
    padded = jnp.concatenate([spread, corr, jnp.zeros_like(corr)], axis=-1)
    w1 = padded.transpose(2, 3, 0, 1, 4).reshape(3 * outputs, -1)
    w2 = conv_second.transpose(2, 3, 0, 1, 4).reshape(3 * outputs, -1)

    kernel = functools.partial(
        compute_kernel, planes=planes, columns=columns, depth_count=depth_count, row_count=row_count
    )
    out = pl.pallas_call(
        kernel,
        out_shape=jax.ShapeDtypeStruct((planes, outputs, lanes), BF16),
        in_specs=[pl.BlockSpec(memory_space=pltpu.VMEM)] * 7,
        out_specs=pl.BlockSpec(memory_space=pltpu.VMEM),
        scratch_shapes=[
            pltpu.VMEM((6, 128, lanes), BF16),
            pltpu.VMEM((4, 32, lanes), F32),
            pltpu.VMEM((4, (planes + 4) * v, lanes), F32),
            pltpu.VMEM((4, (planes + 4) * v, lanes), F32),
            pltpu.VMEM((3, v, 32, lanes), F32),
            pltpu.VMEM((3, v, 32, lanes), F32),
            pltpu.VMEM((3, v, 32, lanes), F32),
            pltpu.VMEM((2, 3, 48, lanes), F32),
            pltpu.VMEM((planes + 4, 240, lanes), BF16),
            pltpu.VMEM((planes + 2, 96, lanes), BF16),
        ],
        compiler_params=pltpu.CompilerParams(vmem_limit_bytes=48 * 1024 * 1024),
        name="volume_and_convolutions",
    )(gathered, far, near, w1, w2, bias_first[:, None], bias_second[:, None])
    out = out.reshape(planes, outputs, b, m, columns).transpose(2, 0, 3, 1, 4)
    return out.reshape(b, planes, m, outputs * columns)


def solution(mesh):
    in_specs = (
        P(None, "rows", None),
        P(None, None, "rows", None),
        P(None, None, "depth", "rows"),
        P(None, None, "depth", "rows", None),
        P(),
        P(),
        P(),
        P(),
    )
    out_specs = P(None, "depth", "rows", None)
    return jax.shard_map(body, mesh=mesh, in_specs=in_specs, out_specs=out_specs, check_vma=False)
```

```python
import functools

import jax
import jax.numpy as jnp
from jax import lax
from jax.experimental import pallas as pl
from jax.experimental.pallas import tpu as pltpu
from jax.sharding import PartitionSpec as P

F32 = jnp.float32
BF16 = jnp.bfloat16


def pack_features(rows, groups, per_group, columns):
    b, v, m, _ = rows.shape
    x = rows.reshape(b, v, m, groups, per_group, columns)
    return x.transpose(1, 4, 3, 2, 0, 5).reshape(v * per_group * groups, b * m * columns)


def pack_blend(weight):
    b, v, p, m, w = weight.shape
    return weight.transpose(2, 1, 3, 0, 4).reshape(p * v, b * m * w)


def compute_kernel(
    own_ref, far_ref, near_ref, w1_ref, w2_ref, b1_ref, b2_ref, out_ref,
    src_ref, rf_ref, tm_ref, tp_ref, e0_ref, dm_ref, dp_ref, vf_ref, v_ref, h_ref,
    *, planes, columns, depth_count, row_count,
):
    q = lax.axis_index("rows")
    core = q % 2
    depth = lax.axis_index("depth")
    lanes = 4 * columns
    views = 4
    first = depth == 0
    last = depth == depth_count - 1

    lane = lax.broadcasted_iota(jnp.int32, (1, lanes), 1)
    col = lane % columns
    second = lane >= lanes // 2
    scene = (lane // columns) % 2 == 1

    src_ref[0] = far_ref[0:128]
    src_ref[1] = near_ref[0]
    src_ref[2] = own_ref[0, 0:128]
    src_ref[3] = own_ref[1, 0:128]
    src_ref[4] = near_ref[1]
    src_ref[5] = far_ref[128:256]
    half = lax.broadcasted_iota(jnp.int32, (8, 128), 1) < 64
    for r in range(4):
        rest = far_ref[256:336] if r in (0, 3) else own_ref[r - 1, 128:208]
        rest = rest.astype(F32)
        rf_ref[r] = rest[0:32]
        for i in range((planes + 4) * views // 8):
            w = rest[32 + 8 * i : 40 + 8 * i]
            o = rest[72:80, 128 * i : 128 * i + 128]
            turned = pltpu.roll(o, 64, 1)
            b0 = jnp.where(half, o, turned)
            b1 = jnp.where(half, turned, o)
            tiles = lanes // 128
            below = jnp.where(scene, jnp.concatenate([b1] * tiles, axis=1), jnp.concatenate([b0] * tiles, axis=1)) < -0.5
            tm_ref[r, 8 * i : 8 * i + 8, :] = jnp.where(below, w, 0.0)
            tp_ref[r, 8 * i : 8 * i + 8, :] = jnp.where(below, 0.0, 1.0 - w)

    for k in range(3):
        base = rf_ref[core + k]
        for v in range(views):
            rows = slice(32 * v, 32 * v + 32)
            middle = src_ref[core + k + 1, rows, :].astype(F32)
            e0_ref[k, v] = middle - base
            dm_ref[k, v] = src_ref[core + k, rows, :].astype(F32) - middle
            dp_ref[k, v] = src_ref[core + k + 2, rows, :].astype(F32) - middle

    def mixed(upper, lower):
        return pltpu.roll(jnp.where(second, upper, lower), lanes // 2, 1)

    def volume_planes(pair):
        outside = first if pair == 0 else last if pair == planes // 2 + 1 else False
        row = 8 * pair
        for k in range(3):
            missing = outside
            if k == 0:
                missing = missing | (q == 0)
            if k == 2:
                missing = missing | (q == row_count - 1)
            keep = jnp.where(missing, 0.0, 1.0).astype(F32)
            for i in range(lanes // 128):
                cols = slice(128 * i, 128 * i + 128)
                tm = tm_ref[core + k, row : row + 8, cols]
                tp = tp_ref[core + k, row : row + 8, cols]
                base = rf_ref[core + k, :, cols]
                for t in range(2):
                    total = jnp.zeros((32, 128), F32)
                    squares = jnp.zeros((32, 128), F32)
                    for v in range(views):
                        n = views * t + v
                        e = e0_ref[k, v, :, cols] + tm[n : n + 1] * dm_ref[k, v, :, cols]
                        e = e + tp[n : n + 1] * dp_ref[k, v, :, cols]
                        total = total + e
                        squares = squares + e * e
                    spread = squares * (0.2 * keep) - total * total * (0.04 * keep)
                    product = base * (total + 4.0 * base)
                    corr = (product[0:8] + product[8:16] + product[16:24] + product[24:32]) * keep
                    vf_ref[pair % 2, t, k, 0:32, cols] = spread
                    vf_ref[pair % 2, t, k, 32:40, cols] = corr
        for t in range(2):
            p = 2 * pair + t
            for k in range(3):
                v_ref[p, 96 * k : 96 * k + 48, :] = vf_ref[pair % 2, t, k].astype(BF16)
            for k in range(2):
                between = mixed(vf_ref[pair % 2, t, k], vf_ref[pair % 2, t, k + 1])
                v_ref[p, 96 * k + 48 : 96 * k + 96, :] = between.astype(BF16)

    vf_ref[:, :, :, 40:48, :] = jnp.zeros((2, 2, 3, 8, lanes), F32)

    def shifted_sum(parts, width):
        column = jnp.concatenate([col] * (width // lanes), axis=1)
        left = jnp.where(column == 0, 0.0, pltpu.roll(parts[0:32], 1, 1))
        right = jnp.where(column == columns - 1, 0.0, pltpu.roll(parts[64:96], width - 1, 1))
        return parts[32:64] + left + right

    inside = jnp.concatenate(
        [
            jnp.where(second | (q != 0), 1.0, 0.0),
            jnp.where(second & (q == row_count - 1), 0.0, 1.0),
        ],
        axis=1,
    )

    def hidden_plane(p):
        upper = jnp.concatenate([v_ref[p + a, 0:144, :] for a in range(3)], axis=0)
        lower = jnp.concatenate([v_ref[p + a, 96:240, :] for a in range(3)], axis=0)
        taps = jnp.concatenate([upper, lower], axis=1)
        parts = jnp.dot(w1_ref[...], taps, preferred_element_type=F32)
        keep = inside
        if p == 0:
            keep = keep * jnp.where(first, 0.0, 1.0).astype(F32)
        if p == planes + 1:
            keep = keep * jnp.where(last, 0.0, 1.0).astype(F32)
        hidden = jnp.maximum(shifted_sum(parts, 2 * lanes) + b1_ref[...], 0.0) * keep
        above = hidden[:, :lanes]
        below = hidden[:, lanes:]
        h_ref[p, 0:32, :] = above.astype(BF16)
        h_ref[p, 32:64, :] = mixed(above, below).astype(BF16)
        h_ref[p, 64:96, :] = below.astype(BF16)

    def out_plane(p):
        taps = jnp.concatenate([h_ref[p + a] for a in range(3)], axis=0)
        parts = jnp.dot(w2_ref[...], taps, preferred_element_type=F32)
        out_ref[p] = (shifted_sum(parts, lanes) + b2_ref[...]).astype(BF16)

    for pair in range(planes // 2 + 2):
        volume_planes(pair)
        if pair >= 1:
            hidden_plane(2 * pair - 2)
            hidden_plane(2 * pair - 1)
        if pair >= 2:
            out_plane(2 * pair - 4)
            out_plane(2 * pair - 3)


def body(ref_feat, src_feat, block_index, blend, conv_first, bias_first, conv_second, bias_second):
    b, v, m, packed = src_feat.shape
    planes, columns = blend.shape[2], blend.shape[4]
    channels = conv_first.shape[4]
    outputs = conv_first.shape[3]
    feat = packed // columns
    groups = channels - feat
    per_group = feat // groups
    depth_count = lax.axis_size("depth")
    row_count = lax.axis_size("rows")
    lanes = b * m * columns
    core = lax.axis_index("rows") % 2

    def send(x, step_depth, step_chip, sign_of_core):
        routes = []
        for d in range(depth_count):
            for r in range(row_count):
                sign = sign_of_core[r % 2]
                to_d, to_r = d + sign * step_depth, r + 2 * sign * step_chip
                if 0 <= to_d < depth_count and 0 <= to_r < row_count:
                    routes.append((d * row_count + r, to_d * row_count + to_r))
        return lax.ppermute(x, ("depth", "rows"), routes)

    rows = planes * v
    offset = (block_index[:, :, :, 0] - lax.axis_index("rows")).astype(BF16)
    offset = offset.transpose(2, 1, 0).reshape(rows // 8, 8, b, 1)
    offset = jnp.broadcast_to(offset, (rows // 8, 8, b, 64)).transpose(1, 0, 2, 3).reshape(8, -1)
    weight = pack_blend(blend)

    def edge(i):
        return jnp.concatenate(
            [weight[8 * i : 8 * i + 8], jnp.pad(offset[:, 128 * i : 128 * i + 128], ((0, 0), (0, lanes - 128)))], axis=0
        )

    low = send(edge(rows // 8 - 1), 1, 0, (1, 1))
    high = send(edge(0), 1, 0, (-1, -1))
    own = jnp.concatenate(
        [
            pack_features(src_feat, groups, per_group, columns),
            pack_features(ref_feat[:, None], groups, per_group, columns),
            low[0:8],
            weight,
            high[0:8],
            jnp.concatenate([low[8:16, 0:128], offset, high[8:16, 0:128]], axis=1),
        ],
        axis=0,
    )
    pairs = [[2 * i, 2 * i + 1] for i in range(row_count // 2)]
    gathered = lax.all_gather(own, "rows", axis_index_groups=pairs)
    rest = lax.dynamic_index_in_dim(gathered, 1 - core, 0, keepdims=False)[128:208]
    far = send(jnp.concatenate([gathered[0, 0:128], gathered[1, 0:128], rest], axis=0), 0, 1, (1, -1))
    near = lax.dynamic_slice_in_dim(far, 128 * (1 - core), 128, 0)
    near = lax.all_gather(near, "rows", axis_index_groups=pairs)

    corr = conv_first[..., :groups] * jnp.asarray(0.0625, BF16)
    spread = conv_first[..., groups:].reshape(3, 3, 3, outputs, groups, per_group)
    spread = spread.swapaxes(4, 5).reshape(3, 3, 3, outputs, feat)
    padded = jnp.concatenate([spread, corr, jnp.zeros_like(corr)], axis=-1)
    w1 = padded.transpose(2, 3, 0, 1, 4).reshape(3 * outputs, -1)
    w2 = conv_second.transpose(2, 3, 0, 1, 4).reshape(3 * outputs, -1)

    kernel = functools.partial(
        compute_kernel, planes=planes, columns=columns, depth_count=depth_count, row_count=row_count
    )
    out = pl.pallas_call(
        kernel,
        out_shape=jax.ShapeDtypeStruct((planes, outputs, lanes), BF16),
        in_specs=[pl.BlockSpec(memory_space=pltpu.VMEM)] * 7,
        out_specs=pl.BlockSpec(memory_space=pltpu.VMEM),
        scratch_shapes=[
            pltpu.VMEM((6, 128, lanes), BF16),
            pltpu.VMEM((4, 32, lanes), F32),
            pltpu.VMEM((4, (planes + 4) * v, lanes), F32),
            pltpu.VMEM((4, (planes + 4) * v, lanes), F32),
            pltpu.VMEM((3, v, 32, lanes), F32),
            pltpu.VMEM((3, v, 32, lanes), F32),
            pltpu.VMEM((3, v, 32, lanes), F32),
            pltpu.VMEM((2, 2, 3, 48, lanes), F32),
            pltpu.VMEM((planes + 4, 240, lanes), BF16),
            pltpu.VMEM((planes + 2, 96, lanes), BF16),
        ],
        compiler_params=pltpu.CompilerParams(vmem_limit_bytes=48 * 1024 * 1024),
        name="volume_and_convolutions",
    )(gathered, far, near, w1, w2, bias_first[:, None], bias_second[:, None])
    out = out.reshape(planes, outputs, m, b, columns).transpose(3, 0, 2, 1, 4)
    return out.reshape(b, planes, m, outputs * columns)


def solution(mesh):
    in_specs = (
        P(None, "rows", None),
        P(None, None, "rows", None),
        P(None, None, "depth", "rows"),
        P(None, None, "depth", "rows", None),
        P(),
        P(),
        P(),
        P(),
    )
    out_specs = P(None, "depth", "rows", None)
    return jax.shard_map(body, mesh=mesh, in_specs=in_specs, out_specs=out_specs, check_vma=False)
```

```python
import functools

import jax
import jax.numpy as jnp
from jax import lax
from jax.experimental import pallas as pl
from jax.experimental.pallas import tpu as pltpu
from jax.sharding import PartitionSpec as P

F32 = jnp.float32
BF16 = jnp.bfloat16


def pack_features(rows, groups, per_group, columns):
    b, v, m, _ = rows.shape
    x = rows.reshape(b, v, m, groups, per_group, columns)
    return x.transpose(1, 4, 3, 2, 0, 5).reshape(v * per_group * groups, b * m * columns)


def pack_blend(weight):
    b, v, p, m, w = weight.shape
    return weight.transpose(2, 1, 3, 0, 4).reshape(p * v, b * m * w)


def compute_kernel(
    own_ref, rest_ref, far_ref, near_ref, w1_ref, w2_ref, b1_ref, b2_ref, out_ref,
    src_ref, rf_ref, tm_ref, tp_ref, e0_ref, dm_ref, dp_ref, vf_ref, v_ref, h_ref, o_ref,
    *, planes, columns, depth_count, row_count,
):
    q = lax.axis_index("rows")
    core = q % 2
    depth = lax.axis_index("depth")
    lanes = 4 * columns
    views = 4
    first = depth == 0
    last = depth == depth_count - 1

    lane = lax.broadcasted_iota(jnp.int32, (1, lanes), 1)
    col = lane % columns
    second = lane >= lanes // 2
    scene = (lane // columns) % 2 == 1

    src_ref[0] = far_ref[0:128]
    src_ref[1] = near_ref[0]
    src_ref[2] = own_ref[0, 0:128]
    src_ref[3] = own_ref[1, 0:128]
    src_ref[4] = near_ref[1]
    src_ref[5] = far_ref[128:256]
    half = lax.broadcasted_iota(jnp.int32, (8, 128), 1) < 64
    for r in range(4):
        rest = far_ref[256:336] if r in (0, 3) else rest_ref[r - 1]
        rest = rest.astype(F32)
        rf_ref[r] = rest[0:32]
        for i in range((planes + 4) * views // 8):
            w = rest[32 + 8 * i : 40 + 8 * i]
            o = rest[72:80, 128 * i : 128 * i + 128]
            turned = pltpu.roll(o, 64, 1)
            b0 = jnp.where(half, o, turned)
            b1 = jnp.where(half, turned, o)
            tiles = lanes // 128
            below = jnp.where(scene, jnp.concatenate([b1] * tiles, axis=1), jnp.concatenate([b0] * tiles, axis=1)) < -0.5
            tm_ref[r, 8 * i : 8 * i + 8, :] = jnp.where(below, w, 0.0)
            tp_ref[r, 8 * i : 8 * i + 8, :] = jnp.where(below, 0.0, 1.0 - w)

    for k in range(3):
        base = rf_ref[core + k]
        for v in range(views):
            rows = slice(32 * v, 32 * v + 32)
            middle = src_ref[core + k + 1, rows, :].astype(F32)
            e0_ref[k, v] = middle - base
            dm_ref[k, v] = src_ref[core + k, rows, :].astype(F32) - middle
            dp_ref[k, v] = src_ref[core + k + 2, rows, :].astype(F32) - middle

    def mixed(upper, lower):
        return pltpu.roll(jnp.where(second, upper, lower), lanes // 2, 1)

    def volume_planes(pair):
        outside = first if pair == 0 else last if pair == planes // 2 + 1 else False
        row = 8 * pair
        for k in range(3):
            missing = outside
            if k == 0:
                missing = missing | (q == 0)
            if k == 2:
                missing = missing | (q == row_count - 1)
            keep = jnp.where(missing, 0.0, 1.0).astype(F32)
            for i in range(lanes // 128):
                cols = slice(128 * i, 128 * i + 128)
                tm = tm_ref[core + k, row : row + 8, cols]
                tp = tp_ref[core + k, row : row + 8, cols]
                base = rf_ref[core + k, :, cols]
                for t in range(2):
                    total = jnp.zeros((32, 128), F32)
                    squares = jnp.zeros((32, 128), F32)
                    for v in range(views):
                        n = views * t + v
                        e = e0_ref[k, v, :, cols] + tm[n : n + 1] * dm_ref[k, v, :, cols]
                        e = e + tp[n : n + 1] * dp_ref[k, v, :, cols]
                        total = total + e
                        squares = squares + e * e
                    spread = squares * (0.2 * keep) - total * total * (0.04 * keep)
                    product = base * (total + 4.0 * base)
                    corr = (product[0:8] + product[8:16] + product[16:24] + product[24:32]) * keep
                    vf_ref[pair % 2, t, k, 0:32, cols] = spread
                    vf_ref[pair % 2, t, k, 32:40, cols] = corr
        for t in range(2):
            p = 2 * pair + t
            for k in range(3):
                v_ref[p, 96 * k : 96 * k + 48, :] = vf_ref[pair % 2, t, k].astype(BF16)
            for k in range(2):
                between = mixed(vf_ref[pair % 2, t, k], vf_ref[pair % 2, t, k + 1])
                v_ref[p, 96 * k + 48 : 96 * k + 96, :] = between.astype(BF16)

    vf_ref[:, :, :, 40:48, :] = jnp.zeros((2, 2, 3, 8, lanes), F32)

    def shifted_sum(parts, width):
        column = jnp.concatenate([col] * (width // lanes), axis=1)
        left = jnp.where(column == 0, 0.0, pltpu.roll(parts[0:32], 1, 1))
        right = jnp.where(column == columns - 1, 0.0, pltpu.roll(parts[64:96], width - 1, 1))
        return parts[32:64] + left + right

    inside = jnp.concatenate(
        [
            jnp.where(second | (q != 0), 1.0, 0.0),
            jnp.where(second & (q == row_count - 1), 0.0, 1.0),
        ],
        axis=1,
    )

    diagonal = lax.broadcasted_iota(jnp.int32, (32, 32), 0) == lax.broadcasted_iota(jnp.int32, (32, 32), 1)
    bias_first = jnp.sum(jnp.where(diagonal, b1_ref[...], 0.0), axis=1, keepdims=True)
    bias_second = jnp.sum(jnp.where(diagonal, b2_ref[...], 0.0), axis=1, keepdims=True)

    def hidden_plane(p):
        upper = jnp.concatenate([v_ref[p + a, 0:144, :] for a in range(3)], axis=0)
        lower = jnp.concatenate([v_ref[p + a, 96:240, :] for a in range(3)], axis=0)
        taps = jnp.concatenate([upper, lower], axis=1)
        parts = jnp.dot(w1_ref[...], taps, preferred_element_type=F32)
        keep = inside
        if p == 0:
            keep = keep * jnp.where(first, 0.0, 1.0).astype(F32)
        if p == planes + 1:
            keep = keep * jnp.where(last, 0.0, 1.0).astype(F32)
        hidden = jnp.maximum(shifted_sum(parts, 2 * lanes) + bias_first, 0.0) * keep
        above = hidden[:, :lanes]
        below = hidden[:, lanes:]
        h_ref[p, 0:32, :] = above.astype(BF16)
        h_ref[p, 32:64, :] = mixed(above, below).astype(BF16)
        h_ref[p, 64:96, :] = below.astype(BF16)

    def out_plane(p):
        taps = jnp.concatenate([h_ref[p + a] for a in range(3)], axis=0)
        parts = jnp.dot(w2_ref[...], taps, preferred_element_type=F32)
        result = shifted_sum(parts, lanes) + bias_second
        for m in range(2):
            for b in range(2):
                at = 32 * ((b * planes + p) * 2 + m)
                start = (2 * m + b) * columns
                o_ref[0, at : at + 32, :] = result[:, start : start + 128]
                o_ref[1, at : at + 32, 0 : columns - 128] = result[:, start + 128 : start + columns]

    for pair in range(planes // 2 + 2):
        volume_planes(pair)
        if pair >= 1:
            hidden_plane(2 * pair - 2)
            hidden_plane(2 * pair - 1)
        if pair >= 2:
            out_plane(2 * pair - 4)
            out_plane(2 * pair - 3)

    for g in range(4 * planes // 8):
        for a in range(8):
            pieces = []
            for j in range(4):
                rows = pl.ds(256 * g + 4 * a + j, 8, stride=32)
                pieces += [o_ref[0, rows, :], o_ref[1, rows, :][:, : columns - 128]]
            out_ref[8 * g : 8 * g + 8, 4 * columns * a : 4 * columns * (a + 1)] = jnp.concatenate(pieces, axis=1).astype(BF16)


def body(ref_feat, src_feat, block_index, blend, conv_first, bias_first, conv_second, bias_second):
    b, v, m, packed = src_feat.shape
    planes, columns = blend.shape[2], blend.shape[4]
    channels = conv_first.shape[4]
    outputs = conv_first.shape[3]
    feat = packed // columns
    groups = channels - feat
    per_group = feat // groups
    depth_count = lax.axis_size("depth")
    row_count = lax.axis_size("rows")
    lanes = b * m * columns
    core = lax.axis_index("rows") % 2

    def send(x, step_depth, step_chip, sign_of_core):
        routes = []
        for d in range(depth_count):
            for r in range(row_count):
                sign = sign_of_core[r % 2]
                to_d, to_r = d + sign * step_depth, r + 2 * sign * step_chip
                if 0 <= to_d < depth_count and 0 <= to_r < row_count:
                    routes.append((d * row_count + r, to_d * row_count + to_r))
        return lax.ppermute(x, ("depth", "rows"), routes)

    rows = planes * v
    offset = (block_index[:, :, :, 0] - lax.axis_index("rows")).astype(BF16)
    offset = offset.transpose(2, 1, 0).reshape(rows // 8, 8, b, 1)
    offset = jnp.broadcast_to(offset, (rows // 8, 8, b, 64)).transpose(1, 0, 2, 3).reshape(8, -1)
    small = jnp.concatenate([pack_blend(blend), jnp.pad(offset, ((0, 0), (0, lanes - offset.shape[1])))], axis=0)
    pairs = [[2 * i, 2 * i + 1] for i in range(row_count // 2)]
    weights = lax.all_gather(small, "rows", axis_index_groups=pairs)
    edge_blend = jnp.where(core == 0, weights[:, rows - 8 : rows], weights[:, 0:8])
    edge_offset = jnp.where(core == 0, weights[:, rows:, 16 * rows - 128 : 16 * rows], weights[:, rows:, 0:128])
    edge_offset = jnp.pad(edge_offset, ((0, 0), (0, 0), (0, lanes - 128)))
    edges = send(jnp.concatenate([edge_blend, edge_offset], axis=1), 1, 0, (1, -1))
    own = jnp.concatenate(
        [
            pack_features(src_feat, groups, per_group, columns),
            pack_features(ref_feat[:, None], groups, per_group, columns),
            edges.reshape(32, lanes),
        ],
        axis=0,
    )
    gathered = lax.all_gather(own, "rows", axis_index_groups=pairs)
    low = gathered[0, 160:192].reshape(2, 16, lanes)
    high = gathered[1, 160:192].reshape(2, 16, lanes)
    offsets = jnp.concatenate([low[:, 8:, :128], weights[:, rows:, : 16 * rows], high[:, 8:, :128]], axis=2)
    rests = jnp.concatenate([gathered[:, 128:160], low[:, 0:8], weights[:, :rows], high[:, 0:8], offsets], axis=1)
    rest = lax.dynamic_index_in_dim(rests, 1 - core, 0, keepdims=False)
    far = send(jnp.concatenate([gathered[0, 0:128], gathered[1, 0:128], rest], axis=0), 0, 1, (1, -1))
    near = lax.dynamic_slice_in_dim(far, 128 * (1 - core), 128, 0)
    near = lax.all_gather(near, "rows", axis_index_groups=pairs)

    corr = conv_first[..., :groups] * jnp.asarray(0.0625, BF16)
    spread = conv_first[..., groups:].reshape(3, 3, 3, outputs, groups, per_group)
    spread = spread.swapaxes(4, 5).reshape(3, 3, 3, outputs, feat)
    padded = jnp.concatenate([spread, corr, jnp.zeros_like(corr)], axis=-1)
    w1 = padded.transpose(2, 3, 0, 1, 4).reshape(3 * outputs, -1)
    w2 = conv_second.transpose(2, 3, 0, 1, 4).reshape(3 * outputs, -1)

    kernel = functools.partial(
        compute_kernel, planes=planes, columns=columns, depth_count=depth_count, row_count=row_count
    )
    out = pl.pallas_call(
        kernel,
        out_shape=jax.ShapeDtypeStruct((b * planes * m, outputs * columns), BF16),
        in_specs=[pl.BlockSpec(memory_space=pltpu.VMEM)] * 8,
        out_specs=pl.BlockSpec(memory_space=pltpu.VMEM),
        scratch_shapes=[
            pltpu.VMEM((6, 128, lanes), BF16),
            pltpu.VMEM((4, 32, lanes), F32),
            pltpu.VMEM((4, (planes + 4) * v, lanes), F32),
            pltpu.VMEM((4, (planes + 4) * v, lanes), F32),
            pltpu.VMEM((3, v, 32, lanes), F32),
            pltpu.VMEM((3, v, 32, lanes), F32),
            pltpu.VMEM((3, v, 32, lanes), F32),
            pltpu.VMEM((2, 2, 3, 48, lanes), F32),
            pltpu.VMEM((planes + 4, 240, lanes), BF16),
            pltpu.VMEM((planes + 2, 96, lanes), BF16),
            pltpu.VMEM((2, b * planes * m * outputs, 128), F32),
        ],
        compiler_params=pltpu.CompilerParams(vmem_limit_bytes=48 * 1024 * 1024),
        name="volume_and_convolutions",
    )(gathered, rests, far, near, w1, w2, bias_first[None, :], bias_second[None, :])
    return out.reshape(b, planes, m, outputs * columns)


def solution(mesh):
    in_specs = (
        P(None, "rows", None),
        P(None, None, "rows", None),
        P(None, None, "depth", "rows"),
        P(None, None, "depth", "rows", None),
        P(),
        P(),
        P(),
        P(),
    )
    out_specs = P(None, "depth", "rows", None)
    return jax.shard_map(body, mesh=mesh, in_specs=in_specs, out_specs=out_specs, check_vma=False)
```

```python
import functools

import jax
import jax.numpy as jnp
from jax import lax
from jax.experimental import pallas as pl
from jax.experimental.pallas import tpu as pltpu
from jax.sharding import PartitionSpec as P

F32 = jnp.float32
BF16 = jnp.bfloat16


def pack_features(rows, groups, per_group, columns):
    b, v, m, _ = rows.shape
    x = rows.reshape(b, v, m, groups, per_group, columns)
    return x.transpose(1, 4, 3, 2, 0, 5).reshape(v * per_group * groups, b * m * columns)


def pack_blend(weight):
    b, v, p, m, w = weight.shape
    return weight.transpose(2, 1, 3, 0, 4).reshape(p * v, b * m * w)


def compute_kernel(
    own_ref, rest_ref, far_ref, near_ref, w1_ref, w2_ref, out_ref,
    src_ref, rf_ref, tm_ref, tp_ref, e0_ref, dm_ref, dp_ref, vf_ref, v_ref, h_ref, o_ref,
    *, planes, columns, depth_count, row_count,
):
    q = lax.axis_index("rows")
    core = q % 2
    depth = lax.axis_index("depth")
    lanes = 4 * columns
    views = 4
    first = depth == 0
    last = depth == depth_count - 1

    lane = lax.broadcasted_iota(jnp.int32, (1, lanes), 1)
    col = lane % columns
    second = lane >= lanes // 2
    scene = (lane // columns) % 2 == 1

    src_ref[0] = far_ref[0:128]
    src_ref[1] = near_ref[0]
    src_ref[2] = own_ref[0, 0:128]
    src_ref[3] = own_ref[1, 0:128]
    src_ref[4] = near_ref[1]
    src_ref[5] = far_ref[128:256]
    half = lax.broadcasted_iota(jnp.int32, (8, 128), 1) < 64
    for r in range(4):
        rest = far_ref[256:336] if r in (0, 3) else rest_ref[r - 1]
        rest = rest.astype(F32)
        rf_ref[r] = rest[0:32]
        for i in range((planes + 4) * views // 8):
            w = rest[32 + 8 * i : 40 + 8 * i]
            o = rest[72:80, 128 * i : 128 * i + 128]
            turned = pltpu.roll(o, 64, 1)
            b0 = jnp.where(half, o, turned)
            b1 = jnp.where(half, turned, o)
            tiles = lanes // 128
            below = jnp.where(scene, jnp.concatenate([b1] * tiles, axis=1), jnp.concatenate([b0] * tiles, axis=1)) < -0.5
            tm_ref[r, 8 * i : 8 * i + 8, :] = jnp.where(below, w, 1.0 - w)
            tp_ref[r, 8 * i : 8 * i + 8, :] = jnp.where(below, 1.0, 0.0)

    for k in range(3):
        base = rf_ref[core + k]
        for v in range(views):
            rows = slice(32 * v, 32 * v + 32)
            middle = src_ref[core + k + 1, rows, :].astype(F32)
            e0_ref[k, v] = middle - base
            dm_ref[k, v] = src_ref[core + k, rows, :].astype(F32) - middle
            dp_ref[k, v] = src_ref[core + k + 2, rows, :].astype(F32) - middle

    def mixed(upper, lower):
        return pltpu.roll(jnp.where(second, upper, lower), lanes // 2, 1)

    def volume_planes(pair):
        outside = first if pair == 0 else last if pair == planes // 2 + 1 else False
        row = 8 * pair
        for k in range(3):
            missing = outside
            if k == 0:
                missing = missing | (q == 0)
            if k == 2:
                missing = missing | (q == row_count - 1)
            keep = jnp.where(missing, 0.0, 1.0).astype(F32)
            for i in range(lanes // 128):
                cols = slice(128 * i, 128 * i + 128)
                tm = tm_ref[core + k, row : row + 8, cols]
                tp = tp_ref[core + k, row : row + 8, cols]
                base = rf_ref[core + k, :, cols]
                for t in range(2):
                    total = jnp.zeros((32, 128), F32)
                    squares = jnp.zeros((32, 128), F32)
                    for v in range(views):
                        n = views * t + v
                        upper = jnp.broadcast_to(tp[n : n + 1], (8, 128)) > 0.5
                        upper = jnp.concatenate([upper] * 4, axis=0)
                        step = jnp.where(upper, dm_ref[k, v, :, cols], dp_ref[k, v, :, cols])
                        e = e0_ref[k, v, :, cols] + tm[n : n + 1] * step
                        total = total + e
                        squares = squares + e * e
                    spread = squares * (0.2 * keep) - total * total * (0.04 * keep)
                    product = base * (total + 4.0 * base)
                    corr = (product[0:8] + product[8:16] + product[16:24] + product[24:32]) * keep
                    vf_ref[pair % 2, t, k, 0:32, cols] = spread
                    vf_ref[pair % 2, t, k, 32:40, cols] = corr
        for t in range(2):
            p = 2 * pair + t
            for k in range(3):
                v_ref[p, 96 * k : 96 * k + 48, :] = vf_ref[pair % 2, t, k].astype(BF16)
            for k in range(2):
                between = mixed(vf_ref[pair % 2, t, k], vf_ref[pair % 2, t, k + 1])
                v_ref[p, 96 * k + 48 : 96 * k + 96, :] = between.astype(BF16)

    vf_ref[:, :, :, 40:48, :] = jnp.ones((2, 2, 3, 8, lanes), F32)
    ones = jnp.ones((16, lanes), BF16)

    def shifted_sum(parts, width):
        column = jnp.concatenate([col] * (width // lanes), axis=1)
        left = jnp.where(column == 0, 0.0, pltpu.roll(parts[0:32], 1, 1))
        right = jnp.where(column == columns - 1, 0.0, pltpu.roll(parts[64:96], width - 1, 1))
        return parts[32:64] + left + right

    inside = jnp.concatenate(
        [
            jnp.where(second | (q != 0), 1.0, 0.0),
            jnp.where(second & (q == row_count - 1), 0.0, 1.0),
        ],
        axis=1,
    )

    def hidden_plane(p):
        upper = jnp.concatenate([v_ref[p + a, 0:144, :] for a in range(3)], axis=0)
        lower = jnp.concatenate([v_ref[p + a, 96:240, :] for a in range(3)], axis=0)
        taps = jnp.concatenate([upper, lower], axis=1)
        parts = jnp.dot(w1_ref[...], taps, preferred_element_type=F32)
        keep = inside
        if p == 0:
            keep = keep * jnp.where(first, 0.0, 1.0).astype(F32)
        if p == planes + 1:
            keep = keep * jnp.where(last, 0.0, 1.0).astype(F32)
        hidden = jnp.maximum(shifted_sum(parts, 2 * lanes), 0.0) * keep
        above = hidden[:, :lanes]
        below = hidden[:, lanes:]
        h_ref[p, 0:32, :] = above.astype(BF16)
        h_ref[p, 32:64, :] = mixed(above, below).astype(BF16)
        h_ref[p, 64:96, :] = below.astype(BF16)

    def out_plane(p):
        taps = jnp.concatenate([h_ref[p + a] for a in range(3)] + [ones], axis=0)
        parts = jnp.dot(w2_ref[...], taps, preferred_element_type=F32)
        result = shifted_sum(parts, lanes)
        for m in range(2):
            for b in range(2):
                at = 32 * ((b * planes + p) * 2 + m)
                start = (2 * m + b) * columns
                o_ref[0, at : at + 32, :] = result[:, start : start + 128]
                o_ref[1, at : at + 32, 0 : columns - 128] = result[:, start + 128 : start + columns]

    for pair in range(planes // 2 + 2):
        volume_planes(pair)
        if pair >= 1:
            hidden_plane(2 * pair - 2)
            hidden_plane(2 * pair - 1)
        if pair >= 2:
            out_plane(2 * pair - 4)
            out_plane(2 * pair - 3)

    for g in range(4 * planes // 8):
        for a in range(8):
            pieces = []
            for j in range(4):
                rows = pl.ds(256 * g + 4 * a + j, 8, stride=32)
                pieces += [o_ref[0, rows, :], o_ref[1, rows, :][:, : columns - 128]]
            values = jnp.concatenate(pieces, axis=1).reshape(4, 2, 4 * columns).astype(BF16)
            out_ref[4 * g : 4 * g + 4, :, 4 * columns * a : 4 * columns * (a + 1)] = values


def body(ref_feat, src_feat, block_index, blend, conv_first, bias_first, conv_second, bias_second):
    b, v, m, packed = src_feat.shape
    planes, columns = blend.shape[2], blend.shape[4]
    channels = conv_first.shape[4]
    outputs = conv_first.shape[3]
    feat = packed // columns
    groups = channels - feat
    per_group = feat // groups
    depth_count = lax.axis_size("depth")
    row_count = lax.axis_size("rows")
    lanes = b * m * columns
    core = lax.axis_index("rows") % 2

    def send(x, step_depth, step_chip, sign_of_core):
        routes = []
        for d in range(depth_count):
            for r in range(row_count):
                sign = sign_of_core[r % 2]
                to_d, to_r = d + sign * step_depth, r + 2 * sign * step_chip
                if 0 <= to_d < depth_count and 0 <= to_r < row_count:
                    routes.append((d * row_count + r, to_d * row_count + to_r))
        return lax.ppermute(x, ("depth", "rows"), routes)

    rows = planes * v
    offset = (block_index[:, :, :, 0] - lax.axis_index("rows")).astype(BF16)
    offset = offset.transpose(2, 1, 0).reshape(rows // 8, 8, b, 1)
    offset = jnp.broadcast_to(offset, (rows // 8, 8, b, 64)).transpose(1, 0, 2, 3).reshape(8, -1)
    small = jnp.concatenate([pack_blend(blend), jnp.pad(offset, ((0, 0), (0, lanes - offset.shape[1])))], axis=0)
    pairs = [[2 * i, 2 * i + 1] for i in range(row_count // 2)]
    weights = lax.all_gather(small, "rows", axis_index_groups=pairs)
    edge_blend = jnp.where(core == 0, weights[:, rows - 8 : rows], weights[:, 0:8])
    edge_offset = jnp.where(core == 0, weights[:, rows:, 16 * rows - 128 : 16 * rows], weights[:, rows:, 0:128])
    edge_offset = jnp.pad(edge_offset, ((0, 0), (0, 0), (0, lanes - 128)))
    edges = send(jnp.concatenate([edge_blend, edge_offset], axis=1), 1, 0, (1, -1))
    own = jnp.concatenate(
        [
            pack_features(src_feat, groups, per_group, columns),
            pack_features(ref_feat[:, None], groups, per_group, columns),
            edges.reshape(32, lanes),
        ],
        axis=0,
    )
    gathered = lax.all_gather(own, "rows", axis_index_groups=pairs)
    low = gathered[0, 160:192].reshape(2, 16, lanes)
    high = gathered[1, 160:192].reshape(2, 16, lanes)
    offsets = jnp.concatenate([low[:, 8:, :128], weights[:, rows:, : 16 * rows], high[:, 8:, :128]], axis=2)
    rests = jnp.concatenate([gathered[:, 128:160], low[:, 0:8], weights[:, :rows], high[:, 0:8], offsets], axis=1)
    rest = lax.dynamic_index_in_dim(rests, 1 - core, 0, keepdims=False)
    far = send(jnp.concatenate([gathered[0, 0:128], gathered[1, 0:128], rest], axis=0), 0, 1, (1, -1))
    near = lax.dynamic_slice_in_dim(far, 128 * (1 - core), 128, 0)
    near = lax.all_gather(near, "rows", axis_index_groups=pairs)

    def split(bias):
        high = lax.reduce_precision(bias, 8, 7)
        middle = lax.reduce_precision(bias - high, 8, 7)
        return jnp.stack([high, middle, bias - high - middle], axis=1).astype(BF16)

    corr = conv_first[..., :groups] * jnp.asarray(0.0625, BF16)
    spread = conv_first[..., groups:].reshape(3, 3, 3, outputs, groups, per_group)
    spread = spread.swapaxes(4, 5).reshape(3, 3, 3, outputs, feat)
    centre = jnp.pad(split(bias_first)[None, None, None], ((1, 1), (1, 1), (1, 1), (0, 0), (0, groups - 3)))
    padded = jnp.concatenate([spread, corr, centre], axis=-1)
    w1 = padded.transpose(2, 3, 0, 1, 4).reshape(3 * outputs, -1)
    w2 = conv_second.transpose(2, 3, 0, 1, 4).reshape(3 * outputs, -1)
    w2 = jnp.concatenate([w2, jnp.pad(split(bias_second), ((outputs, outputs), (0, 13)))], axis=1)

    kernel = functools.partial(
        compute_kernel, planes=planes, columns=columns, depth_count=depth_count, row_count=row_count
    )
    out = pl.pallas_call(
        kernel,
        out_shape=jax.ShapeDtypeStruct((b * planes, m, outputs * columns), BF16),
        in_specs=[pl.BlockSpec(memory_space=pltpu.VMEM)] * 6,
        out_specs=pl.BlockSpec(memory_space=pltpu.VMEM),
        scratch_shapes=[
            pltpu.VMEM((6, 128, lanes), BF16),
            pltpu.VMEM((4, 32, lanes), F32),
            pltpu.VMEM((4, (planes + 4) * v, lanes), F32),
            pltpu.VMEM((4, (planes + 4) * v, lanes), F32),
            pltpu.VMEM((3, v, 32, lanes), F32),
            pltpu.VMEM((3, v, 32, lanes), F32),
            pltpu.VMEM((3, v, 32, lanes), F32),
            pltpu.VMEM((2, 2, 3, 48, lanes), F32),
            pltpu.VMEM((planes + 4, 240, lanes), BF16),
            pltpu.VMEM((planes + 2, 96, lanes), BF16),
            pltpu.VMEM((2, b * planes * m * outputs, 128), F32),
        ],
        compiler_params=pltpu.CompilerParams(vmem_limit_bytes=48 * 1024 * 1024),
        name="volume_and_convolutions",
    )(gathered, rests, far, near, w1, w2)
    return out.reshape(b, planes, m, outputs * columns)


def solution(mesh):
    in_specs = (
        P(None, "rows", None),
        P(None, None, "rows", None),
        P(None, None, "depth", "rows"),
        P(None, None, "depth", "rows", None),
        P(),
        P(),
        P(),
        P(),
    )
    out_specs = P(None, "depth", "rows", None)
    return jax.shard_map(body, mesh=mesh, in_specs=in_specs, out_specs=out_specs, check_vma=False)
```

```python
import functools

import jax
import jax.numpy as jnp
from jax import lax
from jax.experimental import pallas as pl
from jax.experimental.pallas import tpu as pltpu
from jax.sharding import PartitionSpec as P

F32 = jnp.float32
BF16 = jnp.bfloat16


def pack_features(rows, groups, per_group, columns):
    b, v, m, _ = rows.shape
    x = rows.reshape(b, v, m, groups, per_group, columns)
    return x.transpose(1, 4, 3, 2, 0, 5).reshape(v * per_group * groups, b * m * columns)


def pack_blend(weight):
    b, v, p, m, w = weight.shape
    return weight.transpose(2, 1, 3, 0, 4).reshape(p * v, b * m * w)


def compute_kernel(
    own_ref, rest_ref, far_ref, near_ref, w1_ref, w2_ref, out_ref,
    src_ref, rf_ref, tm_ref, tp_ref, e0_ref, dm_ref, dp_ref, vf_ref, v_ref, h_ref, o_ref,
    *, planes, columns, depth_count, row_count,
):
    q = lax.axis_index("rows")
    core = q % 2
    depth = lax.axis_index("depth")
    lanes = 4 * columns
    views = 4
    first = depth == 0
    last = depth == depth_count - 1

    lane = lax.broadcasted_iota(jnp.int32, (1, lanes), 1)
    col = lane % columns
    second = lane >= lanes // 2
    scene = (lane // columns) % 2 == 1

    src_ref[0] = far_ref[0:128]
    src_ref[1] = near_ref[0]
    src_ref[2] = own_ref[0, 0:128]
    src_ref[3] = own_ref[1, 0:128]
    src_ref[4] = near_ref[1]
    src_ref[5] = far_ref[128:256]
    half = lax.broadcasted_iota(jnp.int32, (8, 128), 1) < 64
    for r in range(4):
        rest = far_ref[256:336] if r in (0, 3) else rest_ref[r - 1]
        rest = rest.astype(F32)
        rf_ref[r] = rest[0:32]
        for i in range((planes + 4) * views // 8):
            w = rest[32 + 8 * i : 40 + 8 * i]
            o = rest[72:80, 128 * i : 128 * i + 128]
            turned = pltpu.roll(o, 64, 1)
            b0 = jnp.where(half, o, turned)
            b1 = jnp.where(half, turned, o)
            tiles = lanes // 128
            below = jnp.where(scene, jnp.concatenate([b1] * tiles, axis=1), jnp.concatenate([b0] * tiles, axis=1)) < -0.5
            tm_ref[r, 8 * i : 8 * i + 8, :] = jnp.where(below, w, 1.0 - w)
            tp_ref[r, 8 * i : 8 * i + 8, :] = jnp.where(below, 1.0, 0.0)

    for k in range(3):
        base = rf_ref[core + k]
        for v in range(views):
            rows = slice(32 * v, 32 * v + 32)
            middle = src_ref[core + k + 1, rows, :].astype(F32)
            e0_ref[k, v] = middle - base
            dm_ref[k, v] = src_ref[core + k, rows, :].astype(F32) - middle
            dp_ref[k, v] = src_ref[core + k + 2, rows, :].astype(F32) - middle

    def mixed(upper, lower):
        return pltpu.roll(jnp.where(second, upper, lower), lanes // 2, 1)

    def volume_planes(pair):
        outside = first if pair == 0 else last if pair == planes // 2 + 1 else False
        row = 8 * pair
        for k in range(3):
            missing = outside
            if k == 0:
                missing = missing | (q == 0)
            if k == 2:
                missing = missing | (q == row_count - 1)
            keep = jnp.where(missing, 0.0, 1.0).astype(F32)
            for i in range(lanes // 128):
                cols = slice(128 * i, 128 * i + 128)
                tm = tm_ref[core + k, row : row + 8, cols]
                tp = tp_ref[core + k, row : row + 8, cols]
                base = rf_ref[core + k, :, cols]
                for t in range(2):
                    for v in range(views):
                        n = views * t + v
                        upper = jnp.broadcast_to(tp[n : n + 1], (8, 128)) > 0.5
                        upper = jnp.concatenate([upper] * 4, axis=0)
                        step = jnp.where(upper, dm_ref[k, v, :, cols], dp_ref[k, v, :, cols])
                        e = e0_ref[k, v, :, cols] + tm[n : n + 1] * step
                        total = e if v == 0 else total + e
                        squares = e * e if v == 0 else squares + e * e
                    spread = squares * (0.2 * keep) - total * total * (0.04 * keep)
                    product = base * (total + 4.0 * base)
                    corr = (product[0:8] + product[8:16] + product[16:24] + product[24:32]) * keep
                    vf_ref[pair % 2, t, k, 0:32, cols] = spread
                    vf_ref[pair % 2, t, k, 32:40, cols] = corr
        for t in range(2):
            p = 2 * pair + t
            for k in range(3):
                v_ref[p, 96 * k : 96 * k + 48, :] = vf_ref[pair % 2, t, k].astype(BF16)
            for k in range(2):
                between = mixed(vf_ref[pair % 2, t, k], vf_ref[pair % 2, t, k + 1])
                v_ref[p, 96 * k + 48 : 96 * k + 96, :] = between.astype(BF16)

    vf_ref[:, :, :, 40:48, :] = jnp.ones((2, 2, 3, 8, lanes), F32)
    ones = jnp.ones((16, lanes), BF16)

    def shifted_sum(parts, width):
        column = jnp.concatenate([col] * (width // lanes), axis=1)
        left = jnp.where(column == 0, 0.0, pltpu.roll(parts[0:32], 1, 1))
        right = jnp.where(column == columns - 1, 0.0, pltpu.roll(parts[64:96], width - 1, 1))
        return parts[32:64] + left + right

    inside = jnp.concatenate(
        [
            jnp.where(second | (q != 0), 1.0, 0.0),
            jnp.where(second & (q == row_count - 1), 0.0, 1.0),
        ],
        axis=1,
    )

    def hidden_plane(p):
        upper = jnp.concatenate([v_ref[p + a, 0:144, :] for a in range(3)], axis=0)
        lower = jnp.concatenate([v_ref[p + a, 96:240, :] for a in range(3)], axis=0)
        taps = jnp.concatenate([upper, lower], axis=1)
        parts = jnp.dot(w1_ref[...], taps, preferred_element_type=F32)
        keep = inside
        if p == 0:
            keep = keep * jnp.where(first, 0.0, 1.0).astype(F32)
        if p == planes + 1:
            keep = keep * jnp.where(last, 0.0, 1.0).astype(F32)
        hidden = jnp.maximum(shifted_sum(parts, 2 * lanes), 0.0) * keep
        above = hidden[:, :lanes]
        below = hidden[:, lanes:]
        h_ref[p, 0:32, :] = above.astype(BF16)
        h_ref[p, 32:64, :] = mixed(above, below).astype(BF16)
        h_ref[p, 64:96, :] = below.astype(BF16)

    def out_plane(p):
        taps = jnp.concatenate([h_ref[p + a] for a in range(3)] + [ones], axis=0)
        parts = jnp.dot(w2_ref[...], taps, preferred_element_type=F32)
        result = shifted_sum(parts, lanes)
        for m in range(2):
            for b in range(2):
                at = 32 * ((b * planes + p) * 2 + m)
                start = (2 * m + b) * columns
                o_ref[0, at : at + 32, :] = result[:, start : start + 128]
                o_ref[1, at : at + 32, 0 : columns - 128] = result[:, start + 128 : start + columns]

    for pair in range(planes // 2 + 2):
        volume_planes(pair)
        if pair >= 1:
            hidden_plane(2 * pair - 2)
            hidden_plane(2 * pair - 1)
        if pair >= 2:
            out_plane(2 * pair - 4)
            out_plane(2 * pair - 3)

    for g in range(4 * planes // 8):
        for a in range(8):
            pieces = []
            for j in range(4):
                rows = pl.ds(256 * g + 4 * a + j, 8, stride=32)
                pieces += [o_ref[0, rows, :], o_ref[1, rows, :][:, : columns - 128]]
            values = jnp.concatenate(pieces, axis=1).reshape(4, 2, 4 * columns).astype(BF16)
            out_ref[4 * g : 4 * g + 4, :, 4 * columns * a : 4 * columns * (a + 1)] = values


def body(ref_feat, src_feat, block_index, blend, conv_first, bias_first, conv_second, bias_second):
    b, v, m, packed = src_feat.shape
    planes, columns = blend.shape[2], blend.shape[4]
    channels = conv_first.shape[4]
    outputs = conv_first.shape[3]
    feat = packed // columns
    groups = channels - feat
    per_group = feat // groups
    depth_count = lax.axis_size("depth")
    row_count = lax.axis_size("rows")
    lanes = b * m * columns
    core = lax.axis_index("rows") % 2

    def send(x, step_depth, step_chip, sign_of_core):
        routes = []
        for d in range(depth_count):
            for r in range(row_count):
                sign = sign_of_core[r % 2]
                to_d, to_r = d + sign * step_depth, r + 2 * sign * step_chip
                if 0 <= to_d < depth_count and 0 <= to_r < row_count:
                    routes.append((d * row_count + r, to_d * row_count + to_r))
        return lax.ppermute(x, ("depth", "rows"), routes)

    rows = planes * v
    offset = (block_index[:, :, :, 0] - lax.axis_index("rows")).astype(BF16)
    offset = offset.transpose(2, 1, 0).reshape(rows // 8, 8, b, 1)
    offset = jnp.broadcast_to(offset, (rows // 8, 8, b, 64)).transpose(1, 0, 2, 3).reshape(8, -1)
    small = jnp.concatenate([pack_blend(blend), jnp.pad(offset, ((0, 0), (0, lanes - offset.shape[1])))], axis=0)
    pairs = [[2 * i, 2 * i + 1] for i in range(row_count // 2)]
    weights = lax.all_gather(small, "rows", axis_index_groups=pairs)
    edge_blend = jnp.where(core == 0, weights[:, rows - 8 : rows], weights[:, 0:8])
    edge_offset = jnp.where(core == 0, weights[:, rows:, 16 * rows - 128 : 16 * rows], weights[:, rows:, 0:128])
    edge_offset = jnp.pad(edge_offset, ((0, 0), (0, 0), (0, lanes - 128)))
    edges = send(jnp.concatenate([edge_blend, edge_offset], axis=1), 1, 0, (1, -1))
    own = jnp.concatenate(
        [
            pack_features(src_feat, groups, per_group, columns),
            pack_features(ref_feat[:, None], groups, per_group, columns),
            edges.reshape(32, lanes),
        ],
        axis=0,
    )
    gathered = lax.all_gather(own, "rows", axis_index_groups=pairs)
    low = gathered[0, 160:192].reshape(2, 16, lanes)
    high = gathered[1, 160:192].reshape(2, 16, lanes)
    offsets = jnp.concatenate([low[:, 8:, :128], weights[:, rows:, : 16 * rows], high[:, 8:, :128]], axis=2)
    rests = jnp.concatenate([gathered[:, 128:160], low[:, 0:8], weights[:, :rows], high[:, 0:8], offsets], axis=1)
    rest = lax.dynamic_index_in_dim(rests, 1 - core, 0, keepdims=False)
    far = send(jnp.concatenate([gathered[0, 0:128], gathered[1, 0:128], rest], axis=0), 0, 1, (1, -1))
    near = lax.dynamic_slice_in_dim(far, 128 * (1 - core), 128, 0)
    near = lax.all_gather(near, "rows", axis_index_groups=pairs)

    def split(bias):
        high = lax.reduce_precision(bias, 8, 7)
        middle = lax.reduce_precision(bias - high, 8, 7)
        return jnp.stack([high, middle, bias - high - middle], axis=1).astype(BF16)

    corr = conv_first[..., :groups] * jnp.asarray(0.0625, BF16)
    spread = conv_first[..., groups:].reshape(3, 3, 3, outputs, groups, per_group)
    spread = spread.swapaxes(4, 5).reshape(3, 3, 3, outputs, feat)
    centre = jnp.pad(split(bias_first)[None, None, None], ((1, 1), (1, 1), (1, 1), (0, 0), (0, groups - 3)))
    padded = jnp.concatenate([spread, corr, centre], axis=-1)
    w1 = padded.transpose(2, 3, 0, 1, 4).reshape(3 * outputs, -1)
    w2 = conv_second.transpose(2, 3, 0, 1, 4).reshape(3 * outputs, -1)
    w2 = jnp.concatenate([w2, jnp.pad(split(bias_second), ((outputs, outputs), (0, 13)))], axis=1)

    kernel = functools.partial(
        compute_kernel, planes=planes, columns=columns, depth_count=depth_count, row_count=row_count
    )
    out = pl.pallas_call(
        kernel,
        out_shape=jax.ShapeDtypeStruct((b * planes, m, outputs * columns), BF16),
        in_specs=[pl.BlockSpec(memory_space=pltpu.VMEM)] * 6,
        out_specs=pl.BlockSpec(memory_space=pltpu.VMEM),
        scratch_shapes=[
            pltpu.VMEM((6, 128, lanes), BF16),
            pltpu.VMEM((4, 32, lanes), F32),
            pltpu.VMEM((4, (planes + 4) * v, lanes), F32),
            pltpu.VMEM((4, (planes + 4) * v, lanes), F32),
            pltpu.VMEM((3, v, 32, lanes), F32),
            pltpu.VMEM((3, v, 32, lanes), F32),
            pltpu.VMEM((3, v, 32, lanes), F32),
            pltpu.VMEM((2, 2, 3, 48, lanes), F32),
            pltpu.VMEM((planes + 4, 240, lanes), BF16),
            pltpu.VMEM((planes + 2, 96, lanes), BF16),
            pltpu.VMEM((2, b * planes * m * outputs, 128), F32),
        ],
        compiler_params=pltpu.CompilerParams(vmem_limit_bytes=48 * 1024 * 1024),
        name="volume_and_convolutions",
    )(gathered, rests, far, near, w1, w2)
    return out.reshape(b, planes, m, outputs * columns)


def solution(mesh):
    in_specs = (
        P(None, "rows", None),
        P(None, None, "rows", None),
        P(None, None, "depth", "rows"),
        P(None, None, "depth", "rows", None),
        P(),
        P(),
        P(),
        P(),
    )
    out_specs = P(None, "depth", "rows", None)
    return jax.shard_map(body, mesh=mesh, in_specs=in_specs, out_specs=out_specs, check_vma=False)
```
